32 devices in a mesh: ctx: 32 (over z, y, x, core), head: 1.
Axes of the slice: x: 2, y: 2, z: 4, core: 2. Of those that a mesh axis runs over, the one named last changes fastest.
Arguments:
- queries: bfloat16 [6144, 4096], P('ctx', 'head'), may hold values from -6 to 6
- keys: bfloat16 [6144, 1024], P('ctx', 'head'), may hold values from -6 to 6
- values: bfloat16 [6144, 1024], P('ctx', 'head'), may hold values from -6 to 6
- retrieval: int32 [32], replicated, may hold values 0 or 1
- spans: int32 [2, 32], replicated, may hold values from 64 to 4096, as said below
- out_weight: bfloat16 [4096, 4096], P(None, 'head'), may hold values from -0.09375 to 0.09375
Outputs:
- layer_out: bfloat16 [6144, 4096], P('ctx', 'head')
The draws below stay inside these ranges and needn't reach their ends.
Inputs may be any that keep to these rules, and one draw needn't show every extreme that they name: `spans`: row 0 lies within 64 to 128, row 1 within 2048 to 4096; some head has exactly 128 sink tokens and some head exactly 4096 recent tokens.
All inputs are finite; a program needn't handle non-finite values.
Results may differ from the reference program's by a relative error of at most 0.0075.
Values may be sent and summed in bfloat16 or wider, within the bound.
A program may use at most 192 MiB of HBM per device.

```python
import jax
import jax.numpy as jnp
from jax import lax

D = 4096
QH = 32
KVH = 8
HD = 128
TOK_DEV = 192
SINK = 128
WINDOW = 4096
SEQ = 6144
N_CTX = 32


def draw_queries(key, part):
    drawn = jnp.clip(jax.random.normal(jax.random.fold_in(key, 11), (SEQ, QH * HD), jnp.float32), -6.0, 6.0)
    return drawn.astype(jnp.bfloat16)


def draw_keys(key, part):
    drawn = jnp.clip(jax.random.normal(jax.random.fold_in(key, 12), (SEQ, KVH * HD), jnp.float32), -6.0, 6.0)
    return drawn.astype(jnp.bfloat16)


def draw_spans(key, part):
    sink_sizes = jax.random.randint(jax.random.fold_in(key, 21), (QH,), SINK // 2, SINK + 1)
    window_sizes = jax.random.randint(jax.random.fold_in(key, 22), (QH,), WINDOW // 2, WINDOW + 1)
    picked = jax.random.randint(jax.random.fold_in(key, 23), (2,), 0, QH)
    sink_sizes = sink_sizes.at[picked[0]].set(SINK)
    window_sizes = window_sizes.at[picked[1]].set(WINDOW)
    return jnp.stack([sink_sizes, window_sizes]).astype(jnp.int32)


def place_ends(values, stream_key, least, high):
    extent = values.shape
    place = [jax.random.randint(jax.random.fold_in(stream_key, axis), (), 0, extent[axis]) for axis in range(len(extent))]
    values = values.at[tuple(place)].set(least)
    longest = extent.index(max(extent))
    place[longest] = (place[longest] + 1) % extent[longest]
    return values.at[tuple(place)].set(high)


def block_scale(own_key, extent, split, smallest, high):
    def one(position, blocks):
        heights = jax.random.uniform(jax.random.fold_in(jax.random.fold_in(own_key, 6), position), (blocks,), jnp.float32, smallest / len(split), high / len(split))
        return jnp.repeat(jnp.exp(heights), extent[position] // blocks).reshape((-1,) + (1,) * (len(extent) - position - 1))

    loudness = one(*split[0])
    for cut in split[1:]:
        loudness = loudness * one(*cut)
    return loudness


def scatter_about(stream_key, dims, width, bound, cuts=(), held_as=jnp.bfloat16):
    drawn = jax.random.normal(stream_key, dims, jnp.float32) * width
    if len(cuts) > 0:
        drawn = block_scale(stream_key, dims, cuts, -0.22, 0.18) * drawn
    return jnp.clip(drawn, min=-bound, max=bound).astype(held_as)


def setup_inputs(seed: int = 0) -> dict:
    streams_of = jax.random.split(jax.random.key(seed), 7)
    queries = draw_queries(jax.random.fold_in(streams_of[6], 71), 0)
    keys = draw_keys(jax.random.fold_in(streams_of[6], 71), 0)
    values = scatter_about(streams_of[2], (SEQ, KVH * HD), 1.0, 6.0, ((0, 32),))
    retrieval = place_ends((jax.random.randint(streams_of[3], (QH,), 0, 2) < 1).astype(jnp.int32), jax.random.fold_in(streams_of[3], 1), 0, 1)
    spans = draw_spans(jax.random.fold_in(streams_of[6], 71), 0)
    out_weight = scatter_about(streams_of[5], (D, D), D ** -0.5, 0.09375)
    return dict(queries=queries, keys=keys, values=values, retrieval=retrieval, spans=spans, out_weight=out_weight)


def attend_block(queries_block, offset, keys, values, retrieval, spans):
    row_count = queries_block.shape[0]
    group_size = QH // KVH
    query_heads = queries_block.reshape(row_count, KVH, group_size, HD).astype(jnp.float32)
    key_heads = keys.reshape(SEQ, KVH, HD).astype(jnp.float32)
    value_heads = values.reshape(SEQ, KVH, HD).astype(jnp.float32)
    scores = jnp.einsum("qgjd,kgd->qgjk", query_heads, key_heads) * (HD ** -0.5)
    query_pos = offset + jnp.arange(row_count, dtype=jnp.int32)
    key_pos = jnp.arange(SEQ, dtype=jnp.int32)
    retrieval_heads = retrieval.reshape(KVH, group_size) > 0
    sink_sizes = spans[0].reshape(KVH, group_size)
    window_sizes = spans[1].reshape(KVH, group_size)
    gap = query_pos[:, None] - key_pos[None, :]
    reach = retrieval_heads[None, :, :, None] | (key_pos[None, None, None, :] < sink_sizes[None, :, :, None])
    reach = reach | (gap[:, None, None, :] < window_sizes[None, :, :, None])
    allowed = (gap >= 0)[:, None, None, :] & reach
    masked = jnp.where(allowed, scores, -1e30)
    peaks = jnp.max(masked, axis=-1, keepdims=True)
    weights = jnp.where(allowed, jnp.exp(masked - peaks), 0.0)
    totals = jnp.sum(weights, axis=-1)
    rounded = lax.optimization_barrier(weights.astype(jnp.bfloat16)).astype(jnp.float32)
    mixed = jnp.einsum("qgjk,kgd->qgjd", rounded, value_heads) / totals[..., None]
    return mixed.reshape(row_count, QH * HD).astype(jnp.bfloat16)


def reference(queries, keys, values, retrieval, spans, out_weight):
    blocks = queries.reshape(N_CTX, TOK_DEV, QH * HD)
    offsets = jnp.arange(N_CTX, dtype=jnp.int32) * TOK_DEV

    def one_block(pair):
        return attend_block(pair[0], pair[1], keys, values, retrieval, spans)

    attended = lax.map(one_block, (blocks, offsets)).reshape(SEQ, QH * HD)
    return jnp.dot(attended, out_weight, preferred_element_type=jnp.float32).astype(jnp.bfloat16)
```

```python
import functools

import jax
import jax.numpy as jnp
from jax import lax
from jax.experimental import pallas as pl
from jax.experimental.pallas import tpu as pltpu
from jax.sharding import PartitionSpec as P

HD = 128
LOG2E = 1.4426950408889634
MASKED = -1e30
FLOOR = -1e29
FAR = 1 << 29
LEAST_RECENT = 2048
MOST_SINK = 128
W_SLOTS = 4
MESH = pl.DeviceIdType.MESH


def across(a, b, size):
    if size & (size - 1):
        return (a + b) % size
    total = 0
    bit = 1
    while bit < size:
        x, y = (a // bit) % 2, (b // bit) % 2
        total = total + bit * (x + y - 2 * x * y)
        bit *= 2
    return total


def back(a, b, size):
    if size & (size - 1):
        return (a + size - b) % size
    return across(a, b, size)


def layer_kernel(
    planes, members, rows, group, fused,
    q_hbm, k_hbm, v_hbm, retrieval_ref, spans_ref, *rest,
):
    if fused:
        w_hbm, out_ref, *rest = rest
    else:
        out_ref, *rest = rest
    (q_all, keys, values, peak, total, accum, done, feats, kv_in, kv_out, q_in, q_out, near_out, o_in, o_out, *rest) = rest
    block = members * rows
    width = group * HD
    scale = (HD ** -0.5) * LOG2E
    me = lax.axis_index("ctx")
    plane, member = me // members, me % members
    first_head = lax.axis_index("head") * (members * group) + member * group
    sinks = [spans_ref[0, first_head + h] for h in range(group)]
    windows = [
        jnp.where(retrieval_ref[first_head + h] > 0, FAR, spans_ref[1, first_head + h]) for h in range(group)
    ]
    has_below, has_above = plane > 0, plane < planes - 1

    def lanes(index, count):
        return pl.ds(pl.multiple_of(index * count, count), count)

    def span_of(index, count):
        return pl.ds(pl.multiple_of(index * count, rows), count)

    if fused:
        w_buf, product, w_sem = rest

        def load_w(step):
            owner = back(member, members - 1 - step, members)
            return pltpu.make_async_copy(
                w_hbm.at[lanes(owner, width), :], w_buf.at[step % W_SLOTS], w_sem.at[step % W_SLOTS]
            )

    own_rows = span_of(me, rows)

    def own_kv(c):
        source, target = ((k_hbm, keys), (v_hbm, values))[c]
        return pltpu.make_async_copy(
            source.at[:, lanes(member, HD)], target.at[own_rows, :], kv_in.at[0, member, c]
        )

    def own_q(h):
        return pltpu.make_async_copy(
            q_hbm.at[:, lanes(member * group + h, HD)],
            q_all.at[span_of(member * group + h, rows), :],
            q_in.at[member, h],
        )

    def near_kv(peer, c):
        source, target = ((k_hbm, keys), (v_hbm, values))[c]
        return pltpu.make_async_remote_copy(
            src_ref=source.at[:, lanes(peer, HD)],
            dst_ref=target.at[own_rows, :],
            send_sem=near_out.at[peer, c],
            recv_sem=kv_in.at[0, member, c],
            device_id={"ctx": plane * members + peer},
            device_id_type=MESH,
        )

    def near_q(peer, h):
        return pltpu.make_async_remote_copy(
            src_ref=q_hbm.at[:, lanes(peer * group + h, HD)],
            dst_ref=q_all.at[span_of(member * group + h, rows), :],
            send_sem=q_out.at[peer, h],
            recv_sem=q_in.at[member, h],
            device_id={"ctx": plane * members + peer},
            device_id_type=MESH,
        )

    def up_kv(step, peer, c):
        target = (keys, values)[c]
        piece = span_of((plane - step) * members + peer, rows)
        return pltpu.make_async_remote_copy(
            src_ref=target.at[piece, :],
            dst_ref=target.at[piece, :],
            send_sem=kv_out.at[step, peer, c],
            recv_sem=kv_in.at[step + 1, peer, c],
            device_id={"ctx": me + members},
            device_id_type=MESH,
        )

    def landed_kv(step, peer, c):
        target = (keys, values)[c]
        piece = target.at[span_of((plane - step) * members + peer, rows), :]
        return pltpu.make_async_copy(piece, piece, kv_in.at[step, peer, c])

    def give_o(peer):
        return pltpu.make_async_remote_copy(
            src_ref=done.at[span_of(peer, rows), :],
            dst_ref=feats.at[:, lanes(member, width)],
            send_sem=o_out.at[peer],
            recv_sem=o_in.at[member],
            device_id={"ctx": plane * members + peer},
            device_id_type=MESH,
        )

    def keep_o():
        return pltpu.make_async_copy(
            done.at[span_of(member, rows), :], feats.at[:, lanes(member, width)], o_in.at[member]
        )

    for c in range(2):
        own_kv(c).start()
    for h in range(group):
        own_q(h).start()
    if fused:
        for step in range(min(W_SLOTS, members)):
            load_w(step).start()

    barrier = pltpu.get_barrier_semaphore()
    for offset in range(1, members):
        peer = across(member, offset, members)
        pl.semaphore_signal(barrier, inc=1, device_id={"ctx": plane * members + peer}, device_id_type=MESH)

    @pl.when(has_below)
    def _():
        pl.semaphore_signal(barrier, inc=1, device_id={"ctx": me - members}, device_id_type=MESH)

    @pl.when(has_above)
    def _():
        pl.semaphore_signal(barrier, inc=1, device_id={"ctx": me + members}, device_id_type=MESH)

    pl.semaphore_wait(barrier, members - 1 + has_below.astype(jnp.int32) + has_above.astype(jnp.int32))

    for offset in range(members - 1, 0, -1):
        peer = across(member, offset, members)
        for c in range(2):
            near_kv(peer, c).start()
    for offset in range(members - 1, 0, -1):
        peer = across(member, offset, members)
        for h in range(group):
            near_q(peer, h).start()

    peak[...] = jnp.full_like(peak, FLOOR)
    total[...] = jnp.zeros_like(total)
    accum[...] = jnp.zeros_like(accum)

    def take_kv(step):
        def one(order, carry):
            peer = back(member, order, members)
            for c in range(2):
                landed_kv(step, peer, c).wait()

            @pl.when(has_above)
            def _():
                for c in range(2):
                    up_kv(step, peer, c).start()

            return carry

        lax.fori_loop(0, members, one, 0)

    def tile(index, start, count, allow):
        key_rows = pl.ds(start, count)

        def head_rows(h):
            return span_of(index * group + h, rows)

        def score(h):
            return lax.dot_general(
                q_all[head_rows(h), :], keys[key_rows, :], (((1,), (1,)), ((), ())),
                preferred_element_type=jnp.float32,
            )

        pending = score(0)
        for h in range(group):
            following = score(h + 1) if h + 1 < group else None
            at = head_rows(h)
            scores = allow(h, pending)
            held = peak[at, :]
            fresh = jnp.maximum(held, jnp.max(scores, axis=-1, keepdims=True))
            peak[at, :] = fresh
            shrink = jnp.exp2((held - fresh) * scale)
            weights = jnp.exp2((scores - jnp.tile(fresh, (1, count // HD))) * scale)
            added = weights[:, :HD]
            for c in range(1, count // HD):
                added = added + weights[:, c * HD:(c + 1) * HD]
            total[at, :] = total[at, :] * shrink + added
            accum[at, :] = accum[at, :] * shrink + jnp.dot(
                weights.astype(jnp.bfloat16), values[key_rows, :], preferred_element_type=jnp.float32
            )
            pending = following

    def gaps(count):
        return lax.broadcasted_iota(jnp.int32, (rows, count), 0) - lax.broadcasted_iota(
            jnp.int32, (rows, count), 1
        )

    def finish(index):
        for h in range(group):
            at = span_of(index * group + h, rows)
            mixed = accum[at, :] / jnp.sum(total[at, :], axis=-1, keepdims=True)
            done[span_of(index, rows), h * HD:(h + 1) * HD] = mixed.astype(jnp.bfloat16)

        @pl.when(index == member)
        def _():
            keep_o().start()

        @pl.when(index != member)
        def _():
            give_o(index).start()

    def own_tile(count):
        def run(index, carry):
            for h in range(group):
                piece = q_all.at[span_of(index * group + h, rows), :]
                pltpu.make_async_copy(piece, piece, q_in.at[index, h]).wait()

            def allow(h, scores):
                return jnp.where(gaps(count) >= -index * rows, scores, MASKED)

            tile(index, pl.multiple_of(plane * block, block), count, allow)

            @pl.when(plane == 0)
            def _():
                finish(index)

            return carry

        return run

    take_kv(0)
    half = members // 2
    if half and half * rows % HD == 0:
        lax.fori_loop(0, half, own_tile(half * rows), 0)
        lax.fori_loop(half, members, own_tile(block), 0)
    else:
        lax.fori_loop(0, members, own_tile(block), 0)

    def far_block(step, carry):
        take_kv(step)
        start = pl.multiple_of((plane - step) * block, block)

        def far_tile(order, inner):
            index = across(member, members - 1 - order, members)

            def allow(h, scores):
                gap = gaps(block)
                near = gap < windows[h] - (step * block + index * rows)
                column = lax.broadcasted_iota(jnp.int32, (rows, MOST_SINK), 1)
                sunk = near[:, :MOST_SINK] | (column < sinks[h] - (plane - step) * block)
                near = jnp.concatenate([sunk, near[:, MOST_SINK:]], axis=1)
                return jnp.where(near, scores, MASKED)

            tile(index, start, block, allow)

            @pl.when(step == plane)
            def _():
                finish(index)

            return inner

        lax.fori_loop(0, members, far_tile, 0)
        return carry

    lax.fori_loop(1, plane + 1, far_block, 0)

    if fused:
        columns = w_buf.shape[2]
        chunk = 512 if columns % 512 == 0 else columns
        product[...] = jnp.zeros_like(product)

        def project(step, carry):
            owner = back(member, members - 1 - step, members)
            piece = feats.at[:, lanes(owner, width)]
            pltpu.make_async_copy(piece, piece, o_in.at[owner]).wait()
            load_w(step).wait()
            slot = step % W_SLOTS
            features = feats[:, lanes(owner, width)]

            def part(c, inner):
                at = lanes(c, chunk)
                product[:, at] = product[:, at] + jnp.dot(
                    features, w_buf[slot, :, at], preferred_element_type=jnp.float32
                )
                return inner

            lax.fori_loop(0, columns // chunk, part, 0)

            @pl.when(step + W_SLOTS < members)
            def _():
                load_w(step + W_SLOTS).start()

            return carry

        lax.fori_loop(0, members, project, 0)
        out_ref[...] = product[...].astype(out_ref.dtype)
    else:
        for source in range(members):
            piece = feats.at[:, source * width:(source + 1) * width]
            pltpu.make_async_copy(piece, piece, o_in.at[source]).wait()
        out_ref[...] = feats[...]

    for offset in range(1, members):
        peer = across(member, offset, members)
        for c in range(2):
            near_kv(peer, c).wait_send()
        for h in range(group):
            near_q(peer, h).wait_send()
        give_o(peer).wait_send()

    @pl.when(has_above)
    def _():
        def sent(step, carry):
            def one(peer, inner):
                for c in range(2):
                    up_kv(step, peer, c).wait_send()
                return inner

            return lax.fori_loop(0, members, one, carry)

        lax.fori_loop(0, plane + 1, sent, 0)


def body(planes, members, fused, queries, keys, values, retrieval, spans, out_weight):
    rows = queries.shape[0]
    group = queries.shape[1] // keys.shape[1]
    width = group * HD
    block = members * rows
    if block > LEAST_RECENT or block % HD or block < MOST_SINK:
        raise ValueError("block size")
    anywhere = pl.BlockSpec(memory_space=pl.ANY)
    smem = pl.BlockSpec(memory_space=pltpu.SMEM)
    stacked = group * block
    scratch = [
        pltpu.VMEM((stacked, HD), jnp.bfloat16),
        pltpu.VMEM((planes * block, HD), jnp.bfloat16),
        pltpu.VMEM((planes * block, HD), jnp.bfloat16),
        pltpu.VMEM((stacked, HD), jnp.float32),
        pltpu.VMEM((stacked, HD), jnp.float32),
        pltpu.VMEM((stacked, HD), jnp.float32),
        pltpu.VMEM((block, width), jnp.bfloat16),
        pltpu.VMEM((rows, members * width), jnp.bfloat16),
        pltpu.SemaphoreType.DMA((planes, members, 2)),
        pltpu.SemaphoreType.DMA((planes, members, 2)),
        pltpu.SemaphoreType.DMA((members, group)),
        pltpu.SemaphoreType.DMA((members, group)),
        pltpu.SemaphoreType.DMA((members, 2)),
        pltpu.SemaphoreType.DMA((members,)),
        pltpu.SemaphoreType.DMA((members,)),
    ]
    operands = [queries, keys, values, retrieval, spans]
    in_specs = [anywhere, anywhere, anywhere, smem, smem]
    columns = members * width
    if fused:
        columns = out_weight.shape[1]
        operands.append(out_weight)
        in_specs.append(anywhere)
        scratch += [
            pltpu.VMEM((min(W_SLOTS, members), width, columns), jnp.bfloat16),
            pltpu.VMEM((rows, columns), jnp.float32),
            pltpu.SemaphoreType.DMA((min(W_SLOTS, members),)),
        ]
    result = pl.pallas_call(
        functools.partial(layer_kernel, planes, members, rows, group, fused),
        out_shape=jax.ShapeDtypeStruct((rows, columns), jnp.bfloat16),
        in_specs=in_specs,
        out_specs=pl.BlockSpec(memory_space=pltpu.VMEM),
        scratch_shapes=scratch,
        compiler_params=pltpu.CompilerParams(
            collective_id=0, has_side_effects=True, vmem_limit_bytes=60 * 2 ** 20
        ),
    )(*operands)
    if fused:
        return result
    features = lax.all_gather(result, "head", axis=1, tiled=True)
    return jnp.dot(features, out_weight, preferred_element_type=jnp.float32).astype(jnp.bfloat16)


def solution(mesh):
    ctx, heads = mesh.shape["ctx"], mesh.shape["head"]

    def step(queries, keys, values, retrieval, spans, out_weight):
        members = keys.shape[1] // HD
        if ctx % members:
            raise ValueError("members")
        return body(ctx // members, members, heads == 1, queries, keys, values, retrieval, spans, out_weight)

    in_specs = (P("ctx", "head"), P("ctx", "head"), P("ctx", "head"), P(), P(), P(None, "head"))
    return jax.shard_map(step, mesh=mesh, in_specs=in_specs, out_specs=P("ctx", "head"), check_vma=False)
```

```python
import functools

import jax
import jax.numpy as jnp
from jax import lax
from jax.experimental import pallas as pl
from jax.experimental.pallas import tpu as pltpu
from jax.sharding import PartitionSpec as P

HD = 128
LOG2E = 1.4426950408889634
MASKED = -1e30
FLOOR = -1e29
FAR = 1 << 29
LEAST_RECENT = 2048
MOST_SINK = 128
W_SLOTS = 4
W_COLUMNS = 1024
CORES = 2
MESH = pl.DeviceIdType.MESH


def across(a, b, size):
    if size & (size - 1):
        return (a + b) % size
    total = 0
    bit = 1
    while bit < size:
        x, y = (a // bit) % 2, (b // bit) % 2
        total = total + bit * (x + y - 2 * x * y)
        bit *= 2
    return total


def back(a, b, size):
    if size & (size - 1):
        return (a + size - b) % size
    return across(a, b, size)


def layer_kernel(
    planes, members, rows, group, fused,
    q_hbm, k_hbm, v_hbm, retrieval_ref, spans_ref, *rest,
):
    if fused:
        w_hbm, out_ref, *rest = rest
    else:
        out_ref, *rest = rest
    (q_all, kv, peak, total, accum, done, feats, gap_ref, near_in, near_out, kv_in, up_out, side_out,
     q_in, q_out, o_in, o_out, *rest) = rest
    chips, half = members // CORES, group // CORES
    block, tall, width = members * rows, half * rows, half * HD
    scale = (HD ** -0.5) * LOG2E
    me = lax.axis_index("ctx")
    plane, member = me // members, me % members
    chip, core = member // CORES, member % CORES
    partner = chip * CORES + (1 - core)
    has_below, has_above = plane > 0, plane < planes - 1
    head_base = lax.axis_index("head") * (members * group)

    def head_of(at_chip, at_core, g):
        return (at_chip * CORES + g) * group + at_core * half

    sinks, windows = [], []
    for g in range(CORES):
        for h in range(half):
            head = head_base + head_of(chip, core, g) + h
            sinks.append(spans_ref[0, head])
            windows.append(jnp.where(retrieval_ref[head] > 0, FAR, spans_ref[1, head]))

    def lanes(start, count):
        return pl.ds(pl.multiple_of(start * HD, HD), count * HD)

    def span_of(index, count):
        return pl.ds(pl.multiple_of(index * rows, rows), count * rows)

    def peer_id(peer):
        return {"ctx": plane * members + peer}

    def remote(source, target, send_sem, recv_sem, device_id):
        return pltpu.make_async_remote_copy(
            src_ref=source, dst_ref=target, send_sem=send_sem, recv_sem=recv_sem,
            device_id=device_id, device_id_type=MESH,
        )

    def kv_piece(g, at_plane, source):
        return kv.at[span_of((g * planes + at_plane) * members + source, 1), :]

    def near_kv(to_chip, g, c):
        source = (k_hbm, v_hbm)[c].at[:, lanes(to_chip * CORES + g, 1)]
        target = kv.at[span_of((g * planes + plane) * members + member, 1), c * HD:(c + 1) * HD]
        return source, target

    def own_kv(g, c):
        return pltpu.make_async_copy(*near_kv(chip, g, c), near_in.at[g, chip, c])

    def give_kv(to_chip, g, c):
        return remote(
            *near_kv(to_chip, g, c), near_out.at[to_chip, g, c], near_in.at[g, chip, c],
            peer_id(to_chip * CORES + core),
        )

    def up_kv(g, step, at_chip):
        piece = kv_piece(g, plane - step, at_chip * CORES + core)
        return remote(
            piece, piece, up_out.at[step, g, at_chip], kv_in.at[step + 1, g, at_chip, 0], {"ctx": me + members}
        )

    def side_kv(g, step, at_chip):
        piece = kv_piece(g, plane - step, at_chip * CORES + core)
        return remote(
            piece, piece, side_out.at[step, g, at_chip], kv_in.at[step, g, at_chip, 1], peer_id(partner)
        )

    def q_piece(peer, head):
        at_chip, at_core = peer // CORES, peer % CORES
        source = q_hbm.at[:, lanes(head_of(at_chip, at_core, head // half) + head % half, 1)]
        return source, q_all.at[span_of(member * group + head, 1), :]

    def own_q(head):
        return pltpu.make_async_copy(*q_piece(member, head), q_in.at[member, head])

    def give_q(peer, head):
        return remote(*q_piece(peer, head), q_out.at[peer, head], q_in.at[member, head], peer_id(peer))

    def o_piece(g, peer):
        return (
            done.at[span_of(peer, 1), g * width:(g + 1) * width],
            feats.at[:, lanes(head_of(chip, core, g), half)],
        )

    def keep_o(g):
        return pltpu.make_async_copy(*o_piece(g, member), o_in.at[member, g])

    def give_o(g, peer):
        return remote(*o_piece(g, peer), o_out.at[peer, g], o_in.at[member, g], peer_id(peer))

    def landed(piece, sem):
        pltpu.make_async_copy(piece, piece, sem).wait()

    if fused:
        w_buf, product, w_sem = rest
        slots = w_buf.shape[0]

        def load_w(step):
            g, order = step // chips, step % chips
            owner = back(chip, chips - 1 - order, chips)
            return pltpu.make_async_copy(
                w_hbm.at[lanes((owner * CORES + g) * group, group), :], w_buf.at[step % slots],
                w_sem.at[step % slots],
            )

    for g in range(CORES):
        for c in range(2):
            own_kv(g, c).start()
    for h in range(group):
        own_q(h).start()

    barrier = pltpu.get_barrier_semaphore()
    for offset in range(1, members):
        peer = across(member, offset, members)
        pl.semaphore_signal(barrier, inc=1, device_id=peer_id(peer), device_id_type=MESH)

    @pl.when(has_below)
    def _():
        pl.semaphore_signal(barrier, inc=1, device_id={"ctx": me - members}, device_id_type=MESH)

    @pl.when(has_above)
    def _():
        pl.semaphore_signal(barrier, inc=1, device_id={"ctx": me + members}, device_id_type=MESH)

    pl.semaphore_wait(barrier, members - 1 + has_below.astype(jnp.int32) + has_above.astype(jnp.int32))

    for g in range(CORES):
        for offset in range(1, chips):
            for c in range(2):
                give_kv(across(chip, offset, chips), g, c).start()
    for offset in range(1, members):
        for h in range(group):
            give_q(across(member, offset, members), h).start()
    if fused:
        for step in range(slots):
            load_w(step).start()

    peak[...] = jnp.full_like(peak, FLOOR)
    total[...] = jnp.zeros_like(total)
    accum[...] = jnp.zeros_like(accum)
    if fused:
        product[...] = jnp.zeros_like(product)
    gap_ref[...] = lax.broadcasted_iota(jnp.int32, (rows, block), 0) - lax.broadcasted_iota(
        jnp.int32, (rows, block), 1
    )

    def raise_own(g):
        def one(order, carry):
            up_kv(g, 0, back(chip, order, chips)).start()
            return carry

        lax.fori_loop(0, chips, one, 0)

    def from_side(g, step):
        def other(order, carry):
            at_chip = back(chip, order, chips)
            landed(kv_piece(g, plane - step, at_chip * CORES + 1 - core), kv_in.at[step, g, at_chip, 1])
            return carry

        lax.fori_loop(0, chips, other, 0)

    def take_own():
        for g in range(CORES):
            def one(order, carry):
                at_chip = back(chip, order, chips)
                piece = kv_piece(g, plane, at_chip * CORES + core)
                for c in range(2):
                    landed(piece.at[:, c * HD:(c + 1) * HD], near_in.at[g, at_chip, c])
                if g == 0:
                    @pl.when(has_above)
                    def _():
                        up_kv(g, 0, at_chip).start()

                side_kv(g, 0, at_chip).start()
                return carry

            lax.fori_loop(0, chips, one, 0)

        @pl.when(has_above & (plane == 0))
        def _():
            raise_own(1)

        for g in range(CORES):
            from_side(g, 0)

    def take(g, step):
        def one(order, carry):
            at_chip = back(chip, order, chips)
            landed(kv_piece(g, plane - step, at_chip * CORES + core), kv_in.at[step, g, at_chip, 0])

            @pl.when(has_above)
            def _():
                up_kv(g, step, at_chip).start()

            side_kv(g, step, at_chip).start()
            return carry

        lax.fori_loop(0, chips, one, 0)
        if g == 0:
            @pl.when(has_above & (step == plane))
            def _():
                raise_own(1)

        from_side(g, step)

    def chain(units):
        def score(unit):
            index, g, start, count, _ = unit
            return lax.dot_general(
                q_all[span_of(index * group + g * half, half), :], kv[pl.ds(start, count), :HD],
                (((1,), (1,)), ((), ())), preferred_element_type=jnp.float32,
            )

        pending = score(units[0])
        for n, (index, g, start, count, allow) in enumerate(units):
            following = score(units[n + 1]) if n + 1 < len(units) else None
            at = span_of(index * group + g * half, half)
            scores = jnp.concatenate(
                [jnp.where(allow(h), pending[h * rows:(h + 1) * rows], MASKED) for h in range(half)], axis=0
            )
            held = peak[at, :]
            fresh = jnp.maximum(held, jnp.max(scores, axis=-1, keepdims=True))
            peak[at, :] = fresh
            shrink = jnp.exp2((held - fresh) * scale)
            weights = jnp.exp2(scores * scale - jnp.tile(fresh * scale, (1, count // HD)))
            added = weights[:, :HD]
            for c in range(1, count // HD):
                added = added + weights[:, c * HD:(c + 1) * HD]
            total[at, :] = total[at, :] * shrink + added
            accum[at, :] = accum[at, :] * shrink + jnp.dot(
                weights.astype(jnp.bfloat16), kv[pl.ds(start, count), HD:], preferred_element_type=jnp.float32
            )
            pending = following

    def finish(g, index):
        for h in range(half):
            at = span_of(index * group + g * half + h, 1)
            mixed = accum[at, :] / jnp.sum(total[at, :], axis=-1, keepdims=True)
            done[span_of(index, 1), (g * half + h) * HD:(g * half + h + 1) * HD] = mixed.astype(jnp.bfloat16)

        @pl.when(index == member)
        def _():
            keep_o(g).start()

        @pl.when(index != member)
        def _():
            give_o(g, index).start()

    def own_tile(index):
        for h in range(group):
            landed(q_all.at[span_of(index * group + h, 1), :], q_in.at[index, h])

        def run(count):
            def allow(h):
                return gap_ref[:, :count] >= -index * rows

            chain([
                (index, g, pl.multiple_of((g * planes + plane) * block, block), count, allow) for g in range(CORES)
            ])

        short = members // 2 * rows
        if short % HD == 0 and members % 2 == 0:
            @pl.when(index < members // 2)
            def _():
                run(short)

            @pl.when(index >= members // 2)
            def _():
                run(block)
        else:
            run(block)

        @pl.when(plane == 0)
        def _():
            for g in range(CORES):
                finish(g, index)

    def far_pair(g, step, pair):
        start = pl.multiple_of((g * planes + plane - step) * block, block)

        def unit(index):
            def allow(h):
                gap = gap_ref[...]
                near = gap < windows[g * half + h] - (step * block + index * rows)
                column = lax.broadcasted_iota(jnp.int32, (rows, MOST_SINK), 1)
                sunk = near[:, :MOST_SINK] | (column < sinks[g * half + h] - (plane - step) * block)
                return jnp.concatenate([sunk, near[:, MOST_SINK:]], axis=1)

            return index, g, start, block, allow

        indices = [across(member, pair * 2 + n, members) for n in range(2)]
        chain([unit(index) for index in indices])

        @pl.when(step == plane)
        def _():
            for index in indices:
                finish(g, index)

    pairs = members // 2
    take_own()

    def first(pair, carry):
        for n in range(2):
            own_tile(across(member, pair * 2 + n, members))

        @pl.when(has_below)
        def _():
            @pl.when(pair == 0)
            def _():
                take(0, 1)

            far_pair(0, 1, pair)

        @pl.when((pair == pairs // 2) & (plane > 1))
        def _():
            take(0, 2)

        return carry

    lax.fori_loop(0, pairs, first, 0)

    def far_pairs(g, step):
        def one(order, carry):
            far_pair(g, step, pairs - 1 - order)
            return carry

        lax.fori_loop(0, pairs, one, 0)

    def project(g):
        columns = w_buf.shape[2]
        chunk = W_COLUMNS if columns % W_COLUMNS == 0 else columns

        def one(order, carry):
            step = g * chips + order
            owner = back(chip, chips - 1 - order, chips)
            for at_core in range(CORES):
                landed(feats.at[:, lanes(head_of(owner, at_core, g), half)], o_in.at[owner * CORES + at_core, g])
            load_w(step).wait()
            slot = step % slots
            features = feats[:, lanes((owner * CORES + g) * group, group)]

            def part(c, inner):
                at = pl.ds(pl.multiple_of(c * chunk, chunk), chunk)
                product[:, at] = product[:, at] + jnp.dot(
                    features, w_buf[slot, :, at], preferred_element_type=jnp.float32
                )
                return inner

            lax.fori_loop(0, columns // chunk, part, 0)

            @pl.when(step + slots < CORES * chips)
            def _():
                load_w(step + slots).start()

            return carry

        lax.fori_loop(0, chips, one, 0)

    def far_first(step, carry):
        @pl.when(step > 2)
        def _():
            take(0, step)

        far_pairs(0, step)
        return carry

    lax.fori_loop(2, plane + 1, far_first, 0)

    def far_second(step, carry):
        if fused:
            @pl.when((step == plane) & (plane == planes - 1))
            def _():
                project(0)

        take(1, step)
        far_pairs(1, step)
        return carry

    lax.fori_loop(1, plane + 1, far_second, 0)

    if fused:
        @pl.when(has_above | (plane == 0))
        def _():
            project(0)

        project(1)
        out_ref[...] = product[...].astype(out_ref.dtype)
    else:
        for g in range(CORES):
            for source in range(members):
                at = lanes(head_of(source // CORES, source % CORES, g), half)
                landed(feats.at[:, at], o_in.at[source, g])
        out_ref[...] = feats[...]

    for g in range(CORES):
        for offset in range(1, chips):
            for c in range(2):
                give_kv(across(chip, offset, chips), g, c).wait_send()
        for offset in range(1, members):
            give_o(g, across(member, offset, members)).wait_send()
    for offset in range(1, members):
        for h in range(group):
            give_q(across(member, offset, members), h).wait_send()

    def sent(step, carry):
        def one(at_chip, inner):
            for g in range(CORES):
                @pl.when(has_above)
                def _():
                    up_kv(g, step, at_chip).wait_send()

                side_kv(g, step, at_chip).wait_send()
            return inner

        return lax.fori_loop(0, chips, one, carry)

    lax.fori_loop(0, plane + 1, sent, 0)


def body(planes, members, fused, queries, keys, values, retrieval, spans, out_weight):
    rows = queries.shape[0]
    group = queries.shape[1] // keys.shape[1]
    chips, half = members // CORES, group // CORES
    block = members * rows
    if block > LEAST_RECENT or block % HD or block < MOST_SINK or group % CORES or members % CORES:
        raise ValueError("block size")
    anywhere = pl.BlockSpec(memory_space=pl.ANY)
    smem = pl.BlockSpec(memory_space=pltpu.SMEM)
    stacked = group * block
    scratch = [
        pltpu.VMEM((stacked, HD), jnp.bfloat16),
        pltpu.VMEM((CORES * planes * block, 2 * HD), jnp.bfloat16),
        pltpu.VMEM((stacked, HD), jnp.float32),
        pltpu.VMEM((stacked, HD), jnp.float32),
        pltpu.VMEM((stacked, HD), jnp.float32),
        pltpu.VMEM((block, group * HD), jnp.bfloat16),
        pltpu.VMEM((rows, members * group * HD), jnp.bfloat16),
        pltpu.VMEM((rows, block), jnp.int32),
        pltpu.SemaphoreType.DMA((CORES, chips, 2)),
        pltpu.SemaphoreType.DMA((chips, CORES, 2)),
        pltpu.SemaphoreType.DMA((planes, CORES, chips, 2)),
        pltpu.SemaphoreType.DMA((planes, CORES, chips)),
        pltpu.SemaphoreType.DMA((planes, CORES, chips)),
        pltpu.SemaphoreType.DMA((members, group)),
        pltpu.SemaphoreType.DMA((members, group)),
        pltpu.SemaphoreType.DMA((members, CORES)),
        pltpu.SemaphoreType.DMA((members, CORES)),
    ]
    operands = [queries, keys, values, retrieval, spans]
    in_specs = [anywhere, anywhere, anywhere, smem, smem]
    columns = members * group * HD
    if fused:
        columns = out_weight.shape[1]
        slots = min(W_SLOTS, members)
        operands.append(out_weight)
        in_specs.append(anywhere)
        scratch += [
            pltpu.VMEM((slots, group * HD, columns), jnp.bfloat16),
            pltpu.VMEM((rows, columns), jnp.float32),
            pltpu.SemaphoreType.DMA((slots,)),
        ]
    result = pl.pallas_call(
        functools.partial(layer_kernel, planes, members, rows, group, fused),
        out_shape=jax.ShapeDtypeStruct((rows, columns), jnp.bfloat16),
        in_specs=in_specs,
        out_specs=pl.BlockSpec(memory_space=pltpu.VMEM),
        scratch_shapes=scratch,
        compiler_params=pltpu.CompilerParams(
            collective_id=0, has_side_effects=True, vmem_limit_bytes=62 * 2 ** 20
        ),
    )(*operands)
    if fused:
        return result
    features = lax.all_gather(result, "head", axis=1, tiled=True)
    return jnp.dot(features, out_weight, preferred_element_type=jnp.float32).astype(jnp.bfloat16)


def solution(mesh):
    ctx, heads = mesh.shape["ctx"], mesh.shape["head"]

    def step(queries, keys, values, retrieval, spans, out_weight):
        members = keys.shape[1] // HD
        if ctx % members:
            raise ValueError("members")
        return body(ctx // members, members, heads == 1, queries, keys, values, retrieval, spans, out_weight)

    in_specs = (P("ctx", "head"), P("ctx", "head"), P("ctx", "head"), P(), P(), P(None, "head"))
    return jax.shard_map(step, mesh=mesh, in_specs=in_specs, out_specs=P("ctx", "head"), check_vma=False)
```

```python
import functools

import jax
import jax.numpy as jnp
from jax import lax
from jax.experimental import pallas as pl
from jax.experimental.pallas import tpu as pltpu
from jax.sharding import PartitionSpec as P

HD = 128
LOG2E = 1.4426950408889634
MASKED = -1e30
FAR = 1 << 29
LEAST_RECENT = 2048
MOST_SINK = 128
W_SLOTS = 4
W_COLUMNS = 4096
CORES = 2
SUBLANES = 8
MESH = pl.DeviceIdType.MESH


def across(a, b, size):
    if size & (size - 1):
        return (a + b) % size
    total = 0
    bit = 1
    while bit < size:
        x, y = (a // bit) % 2, (b // bit) % 2
        total = total + bit * (x + y - 2 * x * y)
        bit *= 2
    return total


def back(a, b, size):
    if size & (size - 1):
        return (a + size - b) % size
    return across(a, b, size)


def layer_kernel(
    planes, members, rows, group, fused,
    q_hbm, k_hbm, v_hbm, retrieval_ref, spans_ref, *rest,
):
    if fused:
        w_hbm, out_ref, *rest = rest
    else:
        out_ref, *rest = rest
    (q_all, kv, turned, peak, total, accum, done, feats, gap_ref, near_in, near_out, kv_in, up_out, side_out,
     q_in, q_out, o_in, o_out, *rest) = rest
    chips, half = members // CORES, group // CORES
    block, wide, width = members * rows, half * rows, half * HD
    scale = (HD ** -0.5) * LOG2E
    me = lax.axis_index("ctx")
    plane, member = me // members, me % members
    chip, core = member // CORES, member % CORES
    partner = chip * CORES + (1 - core)
    has_below, has_above = plane > 0, plane < planes - 1
    head_base = lax.axis_index("head") * (members * group)

    def head_of(at_chip, at_core, g):
        return (at_chip * CORES + g) * group + at_core * half

    sinks, windows = [], []
    for g in range(CORES):
        for h in range(half):
            head = head_base + head_of(chip, core, g) + h
            sinks.append(spans_ref[0, head])
            windows.append(jnp.where(retrieval_ref[head] > 0, FAR, spans_ref[1, head]))

    def lanes(start, count):
        return pl.ds(pl.multiple_of(start * HD, HD), count * HD)

    def span_of(index, count):
        return pl.ds(pl.multiple_of(index * rows, rows), count * rows)

    def peer_id(peer):
        return {"ctx": plane * members + peer}

    def remote(source, target, send_sem, recv_sem, device_id):
        return pltpu.make_async_remote_copy(
            src_ref=source, dst_ref=target, send_sem=send_sem, recv_sem=recv_sem,
            device_id=device_id, device_id_type=MESH,
        )

    def kv_piece(g, at_plane, source):
        return kv.at[span_of((g * planes + at_plane) * members + source, 1), :]

    def near_kv(to_chip, g, c):
        source = (k_hbm, v_hbm)[c].at[:, lanes(to_chip * CORES + g, 1)]
        target = kv.at[span_of((g * planes + plane) * members + member, 1), c * HD:(c + 1) * HD]
        return source, target

    def own_kv(g, c):
        return pltpu.make_async_copy(*near_kv(chip, g, c), near_in.at[g, chip, c])

    def give_kv(to_chip, g, c):
        return remote(
            *near_kv(to_chip, g, c), near_out.at[to_chip, g, c], near_in.at[g, chip, c],
            peer_id(to_chip * CORES + core),
        )

    def up_kv(g, step, at_chip):
        piece = kv_piece(g, plane - step, at_chip * CORES + core)
        return remote(
            piece, piece, up_out.at[step, g, at_chip], kv_in.at[step + 1, g, at_chip, 0], {"ctx": me + members}
        )

    def side_kv(g, step, at_chip):
        piece = kv_piece(g, plane - step, at_chip * CORES + core)
        return remote(
            piece, piece, side_out.at[step, g, at_chip], kv_in.at[step, g, at_chip, 1], peer_id(partner)
        )

    def q_piece(peer, head):
        at_chip, at_core = peer // CORES, peer % CORES
        source = q_hbm.at[:, lanes(head_of(at_chip, at_core, head // half) + head % half, 1)]
        return source, q_all.at[span_of(member * group + head, 1), :]

    def own_q(head):
        return pltpu.make_async_copy(*q_piece(member, head), q_in.at[member, head])

    def give_q(peer, head):
        return remote(*q_piece(peer, head), q_out.at[peer, head], q_in.at[member, head], peer_id(peer))

    def o_piece(g, peer):
        return (
            done.at[span_of(peer, 1), lanes(g * half, half)],
            feats.at[:, lanes(head_of(chip, core, g), half)],
        )

    def keep_o(g):
        return pltpu.make_async_copy(*o_piece(g, member), o_in.at[member, g])

    def give_o(g, peer):
        return remote(*o_piece(g, peer), o_out.at[peer, g], o_in.at[member, g], peer_id(peer))

    def landed(piece, sem):
        pltpu.make_async_copy(piece, piece, sem).wait()

    if fused:
        w_buf, product, w_sem = rest
        slots = w_buf.shape[0]

        def load_w(step):
            g, order = step // chips, step % chips
            owner = back(chip, chips - 1 - order, chips)
            return pltpu.make_async_copy(
                w_hbm.at[lanes((owner * CORES + g) * group, group), :], w_buf.at[step % slots],
                w_sem.at[step % slots],
            )

    for g in range(CORES):
        for c in range(2):
            own_kv(g, c).start()
    for h in range(group):
        own_q(h).start()

    barrier = pltpu.get_barrier_semaphore()
    for offset in range(1, members):
        peer = across(member, offset, members)
        pl.semaphore_signal(barrier, inc=1, device_id=peer_id(peer), device_id_type=MESH)

    @pl.when(has_below)
    def _():
        pl.semaphore_signal(barrier, inc=1, device_id={"ctx": me - members}, device_id_type=MESH)

    @pl.when(has_above)
    def _():
        pl.semaphore_signal(barrier, inc=1, device_id={"ctx": me + members}, device_id_type=MESH)

    pl.semaphore_wait(barrier, members - 1 + has_below.astype(jnp.int32) + has_above.astype(jnp.int32))

    for g in range(CORES):
        for offset in range(1, chips):
            for c in range(2):
                give_kv(across(chip, offset, chips), g, c).start()
    for offset in range(1, members):
        for h in range(group):
            give_q(across(member, offset, members), h).start()
    if fused:
        for step in range(slots):
            load_w(step).start()

    if fused:
        product[...] = jnp.zeros_like(product)
    gap_ref[...] = lax.broadcasted_iota(jnp.int32, (block, wide), 1) % rows - lax.broadcasted_iota(
        jnp.int32, (block, wide), 0
    )

    def raise_own(g):
        def one(order, carry):
            up_kv(g, 0, back(chip, order, chips)).start()
            return carry

        lax.fori_loop(0, chips, one, 0)

    def from_side(g, step):
        def other(order, carry):
            at_chip = back(chip, order, chips)
            landed(kv_piece(g, plane - step, at_chip * CORES + 1 - core), kv_in.at[step, g, at_chip, 1])
            return carry

        lax.fori_loop(0, chips, other, 0)

    def turn_values(g, at_plane):
        at = g * planes + at_plane
        turned[at] = kv[pl.ds(pl.multiple_of(at * block, block), block), HD:].T

    def take_own(g):
        def one(order, carry):
            at_chip = back(chip, order, chips)
            piece = kv_piece(g, plane, at_chip * CORES + core)
            for c in range(2):
                landed(piece.at[:, c * HD:(c + 1) * HD], near_in.at[g, at_chip, c])
            if g == 0:
                @pl.when(has_above)
                def _():
                    up_kv(g, 0, at_chip).start()

            side_kv(g, 0, at_chip).start()
            return carry

        lax.fori_loop(0, chips, one, 0)
        if g == 1:
            @pl.when(has_above & (plane == 0))
            def _():
                raise_own(1)

        from_side(g, 0)
        turn_values(g, plane)

    def take(g, step):
        def one(order, carry):
            at_chip = back(chip, order, chips)
            landed(kv_piece(g, plane - step, at_chip * CORES + core), kv_in.at[step, g, at_chip, 0])

            @pl.when(has_above)
            def _():
                up_kv(g, step, at_chip).start()

            side_kv(g, step, at_chip).start()
            return carry

        lax.fori_loop(0, chips, one, 0)

        @pl.when(has_above & (step == plane) & (g == 0))
        def _():
            raise_own(1)

        from_side(g, step)

    def chain(units, first):
        def score(unit):
            index, g, start, count, _ = unit
            return lax.dot_general(
                kv[pl.ds(start, count), :HD], q_all[span_of(index * group + g * half, half), :],
                (((1,), (1,)), ((), ())), preferred_element_type=jnp.float32,
            )

        pending = score(units[0])
        for n, (index, g, start, count, allowed) in enumerate(units):
            following = score(units[n + 1]) if n + 1 < len(units) else None
            at = index * CORES + g
            scores = jnp.where(allowed, pending, MASKED)
            top = jnp.max(scores, axis=0, keepdims=True)
            fresh = jnp.broadcast_to(top, (SUBLANES, wide))
            if not first:
                held = peak[at]
                fresh = jnp.maximum(held, fresh)
                shrink = jnp.exp2((held - fresh) * scale)
            peak[at] = fresh
            weights = jnp.exp2(scores * scale - fresh[:1] * scale)
            added = jnp.sum(weights.reshape(count // SUBLANES, SUBLANES, wide), axis=0)
            mixed = jnp.dot(
                turned[start // block, :, :count], weights.astype(jnp.bfloat16), preferred_element_type=jnp.float32
            )
            if first:
                total[at] = added
                accum[at] = mixed
            else:
                total[at] = total[at] * shrink + added
                accum[at] = accum[at] * shrink[:1] + mixed
            pending = following

    def finish(g, index):
        at = index * CORES + g
        mixed = (accum[at] / jnp.sum(total[at], axis=0, keepdims=True)).astype(jnp.bfloat16).T
        for h in range(half):
            done[span_of(index, 1), lanes(g * half + h, 1)] = mixed[h * rows:(h + 1) * rows]

        @pl.when(index == member)
        def _():
            keep_o(g).start()

        @pl.when(index != member)
        def _():
            give_o(g, index).start()

    batch = 4 if members % 4 == 0 else 2
    turns, pairs = members // batch, members // 2
    lane = lax.broadcasted_iota(jnp.int32, (1, wide), 1)

    def by_head(values):
        held = jnp.full((1, wide), values[0], jnp.int32)
        for h in range(1, half):
            held = jnp.where(lane >= h * rows, values[h], held)
        return held

    def own_pair(pair):
        indices = [across(member, pair * 2 + n, members) for n in range(2)]
        for index in indices:
            for h in range(group):
                landed(q_all.at[span_of(index * group + h, 1), :], q_in.at[index, h])

        def unit(index, g, count):
            start = pl.multiple_of((g * planes + plane) * block, block)
            return index, g, start, count, gap_ref[:count, :] >= -index * rows

        def run(count):
            chain([unit(index, g, count) for g in range(CORES) for index in indices], True)

        short = members // 2 * rows
        if batch == 4 and short % HD == 0:
            @pl.when(indices[0] < members // 2)
            def _():
                run(short)

            @pl.when(indices[0] >= members // 2)
            def _():
                run(block)
        else:
            run(block)

        @pl.when(plane == 0)
        def _():
            for index in indices:
                for g in range(CORES):
                    finish(g, index)

        @pl.when(has_below & (pair == 0))
        def _():
            take(0, 1)

        @pl.when((plane > 1) & (pair == min(2, pairs - 1)))
        def _():
            take(0, 2)

    def far_batch(g, step, indices):
        start = pl.multiple_of((g * planes + plane - step) * block, block)
        key = lax.broadcasted_iota(jnp.int32, (MOST_SINK, wide), 0)
        sink = by_head([jnp.where(g == 0, sinks[h], sinks[half + h]) for h in range(half)])
        window = by_head([jnp.where(g == 0, windows[h], windows[half + h]) for h in range(half)])

        def unit(index):
            near = gap_ref[...] < window - (step * block + index * rows)
            sunk = near[:MOST_SINK] | (key < sink - (plane - step) * block)
            return index, g, start, block, jnp.concatenate([sunk, near[MOST_SINK:]], axis=0)

        chain([unit(index) for index in indices], False)

        @pl.when(step == plane)
        def _():
            for index in indices:
                finish(g, index)

    def project(g):
        columns = w_buf.shape[2]
        chunk = W_COLUMNS if columns % W_COLUMNS == 0 else columns

        def one(order, carry):
            step = g * chips + order
            owner = back(chip, chips - 1 - order, chips)
            for at_core in range(CORES):
                landed(feats.at[:, lanes(head_of(owner, at_core, g), half)], o_in.at[owner * CORES + at_core, g])
            load_w(step).wait()
            slot = step % slots
            features = feats[:, lanes((owner * CORES + g) * group, group)]

            def part(c, inner):
                at = pl.ds(pl.multiple_of(c * chunk, chunk), chunk)
                product[:, at] = product[:, at] + jnp.dot(
                    features, w_buf[slot, :, at], preferred_element_type=jnp.float32
                )
                return inner

            lax.fori_loop(0, columns // chunk, part, 0)

            @pl.when(step + slots < CORES * chips)
            def _():
                load_w(step + slots).start()

            return carry

        lax.fori_loop(0, chips, one, 0)

    for g in range(CORES):
        take_own(g)

    def item(t, carry):
        g = t // jnp.maximum(plane * turns, 1)
        step = t // turns % jnp.maximum(plane, 1) + 1
        turn = t % turns

        def own(n, inner):
            own_pair(n)
            return inner

        lax.fori_loop(
            jnp.where(t < turns, t * (pairs // turns), 0), jnp.where(t < turns, (t + 1) * (pairs // turns), 0), own, 0
        )

        @pl.when(has_below)
        def _():
            @pl.when(turn == 0)
            def _():
                if fused:
                    @pl.when((g == 1) & (step == plane) & (plane == planes - 1))
                    def _():
                        project(0)

                @pl.when((g == 1) | (step > 2))
                def _():
                    take(g, step)

                turn_values(g, plane - step)

            spot = jnp.where((g == 0) & (step == 1), turn, turns - 1 - turn)
            far_batch(g, step, [across(member, spot * batch + n, members) for n in reversed(range(batch))])

        return carry

    lax.fori_loop(0, jnp.maximum(CORES * plane, 1) * turns, item, 0)

    if fused:
        @pl.when(has_above | (plane == 0))
        def _():
            project(0)

        project(1)
        out_ref[...] = product[...].astype(out_ref.dtype)
    else:
        for g in range(CORES):
            for source in range(members):
                at = lanes(head_of(source // CORES, source % CORES, g), half)
                landed(feats.at[:, at], o_in.at[source, g])
        out_ref[...] = feats[...]

    for g in range(CORES):
        for offset in range(1, chips):
            for c in range(2):
                give_kv(across(chip, offset, chips), g, c).wait_send()
        for offset in range(1, members):
            give_o(g, across(member, offset, members)).wait_send()
    for offset in range(1, members):
        for h in range(group):
            give_q(across(member, offset, members), h).wait_send()

    def sent(step, carry):
        def one(at_chip, inner):
            for g in range(CORES):
                @pl.when(has_above)
                def _():
                    up_kv(g, step, at_chip).wait_send()

                side_kv(g, step, at_chip).wait_send()
            return inner

        return lax.fori_loop(0, chips, one, carry)

    lax.fori_loop(0, plane + 1, sent, 0)


def body(planes, members, fused, queries, keys, values, retrieval, spans, out_weight):
    rows = queries.shape[0]
    group = queries.shape[1] // keys.shape[1]
    chips, half = members // CORES, group // CORES
    block = members * rows
    if block > LEAST_RECENT or block % HD or block < MOST_SINK or group % CORES or members % CORES:
        raise ValueError("block size")
    anywhere = pl.BlockSpec(memory_space=pl.ANY)
    smem = pl.BlockSpec(memory_space=pltpu.SMEM)
    stacked, wide = group * block, half * rows
    scratch = [
        pltpu.VMEM((stacked, HD), jnp.bfloat16),
        pltpu.VMEM((CORES * planes * block, 2 * HD), jnp.bfloat16),
        pltpu.VMEM((CORES * planes, HD, block), jnp.bfloat16),
        pltpu.VMEM((members * CORES, SUBLANES, wide), jnp.float32),
        pltpu.VMEM((members * CORES, SUBLANES, wide), jnp.float32),
        pltpu.VMEM((members * CORES, HD, wide), jnp.float32),
        pltpu.VMEM((block, group * HD), jnp.bfloat16),
        pltpu.VMEM((rows, members * group * HD), jnp.bfloat16),
        pltpu.VMEM((block, wide), jnp.int32),
        pltpu.SemaphoreType.DMA((CORES, chips, 2)),
        pltpu.SemaphoreType.DMA((chips, CORES, 2)),
        pltpu.SemaphoreType.DMA((planes, CORES, chips, 2)),
        pltpu.SemaphoreType.DMA((planes, CORES, chips)),
        pltpu.SemaphoreType.DMA((planes, CORES, chips)),
        pltpu.SemaphoreType.DMA((members, group)),
        pltpu.SemaphoreType.DMA((members, group)),
        pltpu.SemaphoreType.DMA((members, CORES)),
        pltpu.SemaphoreType.DMA((members, CORES)),
    ]
    operands = [queries, keys, values, retrieval, spans]
    in_specs = [anywhere, anywhere, anywhere, smem, smem]
    columns = members * group * HD
    if fused:
        columns = out_weight.shape[1]
        slots = min(W_SLOTS, members)
        operands.append(out_weight)
        in_specs.append(anywhere)
        scratch += [
            pltpu.VMEM((slots, group * HD, columns), jnp.bfloat16),
            pltpu.VMEM((rows, columns), jnp.float32),
            pltpu.SemaphoreType.DMA((slots,)),
        ]
    result = pl.pallas_call(
        functools.partial(layer_kernel, planes, members, rows, group, fused),
        out_shape=jax.ShapeDtypeStruct((rows, columns), jnp.bfloat16),
        in_specs=in_specs,
        out_specs=pl.BlockSpec(memory_space=pltpu.VMEM),
        scratch_shapes=scratch,
        compiler_params=pltpu.CompilerParams(
            collective_id=0, has_side_effects=True, vmem_limit_bytes=62 * 2 ** 20,
        ),
    )(*operands)
    if fused:
        return result
    features = lax.all_gather(result, "head", axis=1, tiled=True)
    return jnp.dot(features, out_weight, preferred_element_type=jnp.float32).astype(jnp.bfloat16)


def solution(mesh):
    ctx, heads = mesh.shape["ctx"], mesh.shape["head"]

    def step(queries, keys, values, retrieval, spans, out_weight):
        members = keys.shape[1] // HD
        if ctx % members:
            raise ValueError("members")
        return body(ctx // members, members, heads == 1, queries, keys, values, retrieval, spans, out_weight)

    in_specs = (P("ctx", "head"), P("ctx", "head"), P("ctx", "head"), P(), P(), P(None, "head"))
    return jax.shard_map(step, mesh=mesh, in_specs=in_specs, out_specs=P("ctx", "head"), check_vma=False)
```

```python
import functools

import jax
import jax.numpy as jnp
from jax import lax
from jax.experimental import pallas as pl
from jax.experimental.pallas import tpu as pltpu
from jax.sharding import PartitionSpec as P

HD = 128
LOG2E = 1.4426950408889634
MASKED = -1e30
FAR = 1 << 29
LEAST_RECENT = 2048
MOST_SINK = 128
W_SLOTS = 4
W_COLUMNS = 4096
CORES = 2
SUBLANES = 8
MESH = pl.DeviceIdType.MESH


def across(a, b, size):
    if size & (size - 1):
        return (a + b) % size
    total = 0
    bit = 1
    while bit < size:
        x, y = (a // bit) % 2, (b // bit) % 2
        total = total + bit * (x + y - 2 * x * y)
        bit *= 2
    return total


def back(a, b, size):
    if size & (size - 1):
        return (a + size - b) % size
    return across(a, b, size)


def layer_kernel(
    planes, members, rows, group, fused,
    q_hbm, k_hbm, v_hbm, retrieval_ref, spans_ref, *rest,
):
    if fused:
        w_hbm, out_ref, *rest = rest
    else:
        out_ref, *rest = rest
    (q_all, kv, turned, peak, total, accum, done, feats, gap_ref, near_in, near_out, kv_in, up_out, side_out,
     q_in, q_out, o_in, o_out, *rest) = rest
    chips, half = members // CORES, group // CORES
    block, wide, width = members * rows, half * rows, half * HD
    scale = (HD ** -0.5) * LOG2E
    me = lax.axis_index("ctx")
    plane, member = me // members, me % members
    chip, core = member // CORES, member % CORES
    partner = chip * CORES + (1 - core)
    has_below, has_above = plane > 0, plane < planes - 1
    head_base = lax.axis_index("head") * (members * group)

    def head_of(at_chip, at_core, g):
        return (at_chip * CORES + g) * group + at_core * half

    sinks, windows = [], []
    for g in range(CORES):
        for h in range(half):
            head = head_base + head_of(chip, core, g) + h
            sinks.append(spans_ref[0, head])
            windows.append(jnp.where(retrieval_ref[head] > 0, FAR, spans_ref[1, head]))

    def lanes(start, count):
        return pl.ds(pl.multiple_of(start * HD, HD), count * HD)

    def span_of(index, count):
        return pl.ds(pl.multiple_of(index * rows, rows), count * rows)

    def peer_id(peer):
        return {"ctx": plane * members + peer}

    def remote(source, target, send_sem, recv_sem, device_id):
        return pltpu.make_async_remote_copy(
            src_ref=source, dst_ref=target, send_sem=send_sem, recv_sem=recv_sem,
            device_id=device_id, device_id_type=MESH,
        )

    def kv_part(g, at_plane, at_core):
        return kv.at[pl.ds((g * planes + at_plane) * chips, chips), at_core]

    def kv_rows(at, count, c):
        taken = kv[pl.ds(at * chips, count // (CORES * rows)), :, :, c * HD:(c + 1) * HD]
        return taken.reshape(count, HD)

    def near_kv(to_chip, g, c):
        source = (k_hbm, v_hbm)[c].at[:, lanes(to_chip * CORES + g, 1)]
        target = kv.at[(g * planes + plane) * chips + chip, core, :, c * HD:(c + 1) * HD]
        return source, target

    def own_kv(g, c):
        return pltpu.make_async_copy(*near_kv(chip, g, c), near_in.at[g, chip, c])

    def give_kv(to_chip, g, c):
        return remote(
            *near_kv(to_chip, g, c), near_out.at[to_chip, g, c], near_in.at[g, chip, c],
            peer_id(to_chip * CORES + core),
        )

    def up_kv(g, step):
        part = kv_part(g, plane - step, core)
        return remote(part, part, up_out.at[step, g], kv_in.at[step + 1, g, 0], {"ctx": me + members})

    def side_kv(g, step):
        part = kv_part(g, plane - step, core)
        return remote(part, part, side_out.at[step, g], kv_in.at[step, g, 1], peer_id(partner))

    def q_piece(peer, head):
        at_chip, at_core = peer // CORES, peer % CORES
        source = q_hbm.at[:, lanes(head_of(at_chip, at_core, head // half) + head % half, 1)]
        return source, q_all.at[span_of(member * group + head, 1), :]

    def own_q(head):
        return pltpu.make_async_copy(*q_piece(member, head), q_in.at[member, head])

    def give_q(peer, head):
        return remote(*q_piece(peer, head), q_out.at[peer, head], q_in.at[member, head], peer_id(peer))

    def o_piece(g, peer):
        return (
            done.at[span_of(peer, 1), lanes(g * half, half)],
            feats.at[:, lanes(head_of(chip, core, g), half)],
        )

    def keep_o(g):
        return pltpu.make_async_copy(*o_piece(g, member), o_in.at[member, g])

    def give_o(g, peer):
        return remote(*o_piece(g, peer), o_out.at[peer, g], o_in.at[member, g], peer_id(peer))

    def landed(piece, sem):
        pltpu.make_async_copy(piece, piece, sem).wait()

    if fused:
        w_buf, product, w_sem = rest
        slots = w_buf.shape[0]

        def load_w(step):
            g, order = step // chips, step % chips
            owner = back(chip, chips - 1 - order, chips)
            return pltpu.make_async_copy(
                w_hbm.at[lanes((owner * CORES + g) * group, group), :], w_buf.at[step % slots],
                w_sem.at[step % slots],
            )

    for g in range(CORES):
        for c in range(2):
            own_kv(g, c).start()
    for h in range(group):
        own_q(h).start()

    barrier = pltpu.get_barrier_semaphore()
    for offset in range(1, members):
        peer = across(member, offset, members)
        pl.semaphore_signal(barrier, inc=1, device_id=peer_id(peer), device_id_type=MESH)

    @pl.when(has_below)
    def _():
        pl.semaphore_signal(barrier, inc=1, device_id={"ctx": me - members}, device_id_type=MESH)

    @pl.when(has_above)
    def _():
        pl.semaphore_signal(barrier, inc=1, device_id={"ctx": me + members}, device_id_type=MESH)

    pl.semaphore_wait(barrier, members - 1 + has_below.astype(jnp.int32) + has_above.astype(jnp.int32))

    for g in range(CORES):
        for offset in range(1, chips):
            for c in range(2):
                give_kv(across(chip, offset, chips), g, c).start()
    for offset in range(1, members):
        for h in range(group):
            give_q(across(member, offset, members), h).start()
    if fused:
        for step in range(slots):
            load_w(step).start()

    if fused:
        product[...] = jnp.zeros_like(product)
    gap_ref[...] = lax.broadcasted_iota(jnp.int32, (block, wide), 1) % rows - lax.broadcasted_iota(
        jnp.int32, (block, wide), 0
    )

    def turn_values(g, at_plane):
        at = g * planes + at_plane
        turned[at] = kv_rows(at, block, 1).T

    def take_own(g):
        def one(order, carry):
            at_chip = back(chip, order, chips)
            for c in range(2):
                landed(
                    kv.at[(g * planes + plane) * chips + at_chip, core, :, c * HD:(c + 1) * HD],
                    near_in.at[g, at_chip, c],
                )
            return carry

        lax.fori_loop(0, chips, one, 0)

        @pl.when(has_above & ((plane == 0) | (g == 0)))
        def _():
            up_kv(g, 0).start()

        side_kv(g, 0).start()
        landed(kv_part(g, plane, 1 - core), kv_in.at[0, g, 1])
        turn_values(g, plane)

    def take(g, step):
        landed(kv_part(g, plane - step, core), kv_in.at[step, g, 0])

        @pl.when(has_above)
        def _():
            up_kv(g, step).start()

        side_kv(g, step).start()

        @pl.when(has_above & (step == plane) & (g == 0))
        def _():
            up_kv(1, 0).start()

        landed(kv_part(g, plane - step, 1 - core), kv_in.at[step, g, 1])

    def chain(units, first):
        def score(unit):
            index, g, at, count, _ = unit
            return lax.dot_general(
                kv_rows(at, count, 0), q_all[span_of(index * group + g * half, half), :],
                (((1,), (1,)), ((), ())), preferred_element_type=jnp.float32,
            )

        pending = score(units[0])
        for n, (index, g, source, count, allowed) in enumerate(units):
            following = score(units[n + 1]) if n + 1 < len(units) else None
            at = index * CORES + g
            scores = jnp.where(allowed, pending, MASKED)
            top = jnp.max(scores, axis=0, keepdims=True)
            fresh = jnp.broadcast_to(top, (SUBLANES, wide))
            if not first:
                held = peak[at]
                fresh = jnp.maximum(held, fresh)
                shrink = jnp.exp2((held - fresh) * scale)
            peak[at] = fresh
            weights = jnp.exp2(scores * scale - fresh[:1] * scale)
            added = jnp.sum(weights.reshape(count // SUBLANES, SUBLANES, wide), axis=0)
            mixed = jnp.dot(
                turned[source, :, :count], weights.astype(jnp.bfloat16), preferred_element_type=jnp.float32
            )
            if first:
                total[at] = added
                accum[at] = mixed
            else:
                total[at] = total[at] * shrink + added
                accum[at] = accum[at] * shrink[:1] + mixed
            pending = following

    def finish(g, index):
        at = index * CORES + g
        mixed = (accum[at] / jnp.sum(total[at], axis=0, keepdims=True)).astype(jnp.bfloat16).T
        for h in range(half):
            done[span_of(index, 1), lanes(g * half + h, 1)] = mixed[h * rows:(h + 1) * rows]

        @pl.when(index == member)
        def _():
            keep_o(g).start()

        @pl.when(index != member)
        def _():
            give_o(g, index).start()

    batch = 4 if members % 4 == 0 else 2
    turns, pairs = members // batch, members // 2
    lane = lax.broadcasted_iota(jnp.int32, (1, wide), 1)

    def by_head(values):
        held = jnp.full((1, wide), values[0], jnp.int32)
        for h in range(1, half):
            held = jnp.where(lane >= h * rows, values[h], held)
        return held

    def own_pair(pair):
        indices = [across(member, pair * 2 + n, members) for n in range(2)]
        for index in indices:
            for h in range(group):
                landed(q_all.at[span_of(index * group + h, 1), :], q_in.at[index, h])

        def unit(index, g, count):
            return index, g, g * planes + plane, count, gap_ref[:count, :] >= -index * rows

        def run(count):
            chain([unit(index, g, count) for g in range(CORES) for index in indices], True)

        short = members // 2 * rows
        if batch == 4 and short % HD == 0:
            @pl.when(indices[0] < members // 2)
            def _():
                run(short)

            @pl.when(indices[0] >= members // 2)
            def _():
                run(block)
        else:
            run(block)

        @pl.when(plane == 0)
        def _():
            for index in indices:
                for g in range(CORES):
                    finish(g, index)

        @pl.when(has_below & (pair == 0))
        def _():
            take(0, 1)

        @pl.when((plane > 1) & (pair == min(2, pairs - 1)))
        def _():
            take(0, 2)

    def far_batch(g, step, indices):
        at = g * planes + plane - step
        key = lax.broadcasted_iota(jnp.int32, (MOST_SINK, wide), 0)
        sink = by_head([jnp.where(g == 0, sinks[h], sinks[half + h]) for h in range(half)])
        window = by_head([jnp.where(g == 0, windows[h], windows[half + h]) for h in range(half)])

        def unit(index):
            near = gap_ref[...] < window - (step * block + index * rows)
            sunk = near[:MOST_SINK] | (key < sink - (plane - step) * block)
            return index, g, at, block, jnp.concatenate([sunk, near[MOST_SINK:]], axis=0)

        chain([unit(index) for index in indices], False)

        @pl.when(step == plane)
        def _():
            for index in indices:
                finish(g, index)

    def project(g):
        columns = w_buf.shape[2]
        chunk = W_COLUMNS if columns % W_COLUMNS == 0 else columns

        def one(order, carry):
            step = g * chips + order
            owner = back(chip, chips - 1 - order, chips)
            for at_core in range(CORES):
                landed(feats.at[:, lanes(head_of(owner, at_core, g), half)], o_in.at[owner * CORES + at_core, g])
            load_w(step).wait()
            slot = step % slots
            features = feats[:, lanes((owner * CORES + g) * group, group)]

            def part(c, inner):
                at = pl.ds(pl.multiple_of(c * chunk, chunk), chunk)
                product[:, at] = product[:, at] + jnp.dot(
                    features, w_buf[slot, :, at], preferred_element_type=jnp.float32
                )
                return inner

            lax.fori_loop(0, columns // chunk, part, 0)

            @pl.when(step + slots < CORES * chips)
            def _():
                load_w(step + slots).start()

            return carry

        lax.fori_loop(0, chips, one, 0)

    for g in range(CORES):
        take_own(g)

    def item(t, carry):
        g = t // jnp.maximum(plane * turns, 1)
        step = t // turns % jnp.maximum(plane, 1) + 1
        turn = t % turns

        def own(n, inner):
            own_pair(n)
            return inner

        lax.fori_loop(
            jnp.where(t < turns, t * (pairs // turns), 0), jnp.where(t < turns, (t + 1) * (pairs // turns), 0), own, 0
        )

        @pl.when(has_below)
        def _():
            @pl.when(turn == 0)
            def _():
                @pl.when((g == 1) | (step > 2))
                def _():
                    take(g, step)

                turn_values(g, plane - step)

            spot = jnp.where((g == 0) & (step == 1), turn, turns - 1 - turn)
            far_batch(g, step, [across(member, spot * batch + n, members) for n in reversed(range(batch))])

        return carry

    lax.fori_loop(0, jnp.maximum(CORES * plane, 1) * turns, item, 0)

    if fused:
        for g in range(CORES):
            project(g)
        out_ref[...] = product[...].astype(out_ref.dtype)
    else:
        for g in range(CORES):
            for source in range(members):
                at = lanes(head_of(source // CORES, source % CORES, g), half)
                landed(feats.at[:, at], o_in.at[source, g])
        out_ref[...] = feats[...]

    for g in range(CORES):
        for offset in range(1, chips):
            for c in range(2):
                give_kv(across(chip, offset, chips), g, c).wait_send()
        for offset in range(1, members):
            give_o(g, across(member, offset, members)).wait_send()
    for offset in range(1, members):
        for h in range(group):
            give_q(across(member, offset, members), h).wait_send()

    def sent(step, carry):
        for g in range(CORES):
            @pl.when(has_above)
            def _():
                up_kv(g, step).wait_send()

            side_kv(g, step).wait_send()
        return carry

    lax.fori_loop(0, plane + 1, sent, 0)


def body(planes, members, fused, queries, keys, values, retrieval, spans, out_weight):
    rows = queries.shape[0]
    group = queries.shape[1] // keys.shape[1]
    chips, half = members // CORES, group // CORES
    block = members * rows
    if block > LEAST_RECENT or block % HD or block < MOST_SINK or group % CORES or members % CORES:
        raise ValueError("block size")
    anywhere = pl.BlockSpec(memory_space=pl.ANY)
    smem = pl.BlockSpec(memory_space=pltpu.SMEM)
    stacked, wide = group * block, half * rows
    scratch = [
        pltpu.VMEM((stacked, HD), jnp.bfloat16),
        pltpu.VMEM((CORES * planes * chips, CORES, rows, 2 * HD), jnp.bfloat16),
        pltpu.VMEM((CORES * planes, HD, block), jnp.bfloat16),
        pltpu.VMEM((members * CORES, SUBLANES, wide), jnp.float32),
        pltpu.VMEM((members * CORES, SUBLANES, wide), jnp.float32),
        pltpu.VMEM((members * CORES, HD, wide), jnp.float32),
        pltpu.VMEM((block, group * HD), jnp.bfloat16),
        pltpu.VMEM((rows, members * group * HD), jnp.bfloat16),
        pltpu.VMEM((block, wide), jnp.int32),
        pltpu.SemaphoreType.DMA((CORES, chips, 2)),
        pltpu.SemaphoreType.DMA((chips, CORES, 2)),
        pltpu.SemaphoreType.DMA((planes, CORES, 2)),
        pltpu.SemaphoreType.DMA((planes, CORES)),
        pltpu.SemaphoreType.DMA((planes, CORES)),
        pltpu.SemaphoreType.DMA((members, group)),
        pltpu.SemaphoreType.DMA((members, group)),
        pltpu.SemaphoreType.DMA((members, CORES)),
        pltpu.SemaphoreType.DMA((members, CORES)),
    ]
    operands = [queries, keys, values, retrieval, spans]
    in_specs = [anywhere, anywhere, anywhere, smem, smem]
    columns = members * group * HD
    if fused:
        columns = out_weight.shape[1]
        slots = min(W_SLOTS, members)
        operands.append(out_weight)
        in_specs.append(anywhere)
        scratch += [
            pltpu.VMEM((slots, group * HD, columns), jnp.bfloat16),
            pltpu.VMEM((rows, columns), jnp.float32),
            pltpu.SemaphoreType.DMA((slots,)),
        ]
    result = pl.pallas_call(
        functools.partial(layer_kernel, planes, members, rows, group, fused),
        out_shape=jax.ShapeDtypeStruct((rows, columns), jnp.bfloat16),
        in_specs=in_specs,
        out_specs=pl.BlockSpec(memory_space=pltpu.VMEM),
        scratch_shapes=scratch,
        compiler_params=pltpu.CompilerParams(
            collective_id=0, has_side_effects=True, vmem_limit_bytes=62 * 2 ** 20,
        ),
    )(*operands)
    if fused:
        return result
    features = lax.all_gather(result, "head", axis=1, tiled=True)
    return jnp.dot(features, out_weight, preferred_element_type=jnp.float32).astype(jnp.bfloat16)


def solution(mesh):
    ctx, heads = mesh.shape["ctx"], mesh.shape["head"]

    def step(queries, keys, values, retrieval, spans, out_weight):
        members = keys.shape[1] // HD
        if ctx % members:
            raise ValueError("members")
        return body(ctx // members, members, heads == 1, queries, keys, values, retrieval, spans, out_weight)

    in_specs = (P("ctx", "head"), P("ctx", "head"), P("ctx", "head"), P(), P(), P(None, "head"))
    return jax.shard_map(step, mesh=mesh, in_specs=in_specs, out_specs=P("ctx", "head"), check_vma=False)
```
